32 devices in a mesh: beam: 2 (over x), tm: 16 (over z, y, core).
Axes of the slice: x: 2, y: 2, z: 4, core: 2. Of those that a mesh axis runs over, the one named last changes fastest.
Arguments:
- voltage: bfloat16 [2, 2, 2097152], P(None, None, ('beam', 'tm')), parts along dimension 2, may hold values from -11 to 11
- delays: int32 [64, 2048], replicated, may hold values from 0 to 96, as said below
- chan_mask: int32 [4096], P('beam'), parts along dimension 0, may hold values 0 or 1
Outputs:
- zscore: float32 [64, 1024], P(None, ('beam', 'tm')), parts along dimension 1
- trial_stats: float32 [3, 128], P(None, 'beam'), parts along dimension 1
The draws below stay inside these ranges and needn't reach their ends.
There are 2 independent parts, one for each index of `beam`. The reference program is written for one: setup_inputs(seed, part) draws one part's arguments, and reference() takes and returns one part's arrays. A program takes and returns all parts, laid end to end along the dimension named above; an argument that names none is the same for every part. Nothing has to cross between parts.
Inputs may be any that keep to these rules, and one draw needn't show every extreme that they name: For each trial the delays never rise from one channel to the next; the last channel's delays are 0, and the first channel's delay of some trial is 96.
All inputs are finite; a program needn't handle non-finite values.
Results may differ from the reference program's by a relative error of at most 0.002.
Values may be sent and summed in bfloat16 or wider, within the bound.
A program may use at most 64 MiB of HBM per device.

```python
import jax
import jax.numpy as jnp
from jax import lax

NCHAN = 2048
TAPS = 16
NDM = 64
SAMPLES = 1048576
MAXD = 96


def draw_voltage(key, part):
    noise_key = jax.random.fold_in(jax.random.fold_in(key, 11), 0)
    position = jnp.arange(SAMPLES, dtype=jnp.float32) / SAMPLES
    envelope = jnp.exp(0.5 * jnp.log(3.5) * position)
    values = jnp.clip(jax.random.normal(noise_key, (2, 2, SAMPLES), jnp.float32) * envelope, -11.0, 11.0)
    return values.astype(jnp.bfloat16)


def draw_delays(key, part):
    size_key, pick_key = jax.random.split(jax.random.fold_in(key, 23))
    reaches = jax.random.randint(size_key, (NDM,), 0, MAXD + 1)
    chosen = jax.random.randint(pick_key, (), 0, NDM)
    reaches = jnp.where(jnp.arange(NDM, dtype=jnp.int32) == chosen, MAXD, reaches)
    channel = jnp.arange(NCHAN, dtype=jnp.int32)
    scale_unit = max(1, (NCHAN - 1) * 3 * NCHAN // 4096)
    chan_curve = (NCHAN - 1 - channel) * (3 * NCHAN - channel) // scale_unit
    top_value = (NCHAN - 1) * 3 * NCHAN // scale_unit
    return (reaches[:, None] * chan_curve[None, :] // top_value).astype(jnp.int32)


def plant(array, rng, least, high):
    shape = array.shape
    place = [jax.random.randint(jax.random.fold_in(rng, axis), (), 0, shape[axis]) for axis in range(len(shape))]
    array = array.at[tuple(place)].set(least)
    longest = shape.index(max(shape))
    place[longest] = (place[longest] + 1) % shape[longest]
    return array.at[tuple(place)].set(high)


def setup_inputs(seed: int = 0, part: int = 0) -> dict:
    key_of = jax.random.split(jax.random.key(seed), 4)
    part_splits = jax.random.split(jax.random.fold_in(key_of[3], part), 4)
    return {
        "voltage": draw_voltage(jax.random.fold_in(jax.random.fold_in(key_of[3], part), 71), part),
        "delays": draw_delays(jax.random.fold_in(key_of[3], 71), part),
        "chan_mask": plant((jax.random.randint(part_splits[2], (NCHAN,), 0, 8) < 7).astype(jnp.int32), jax.random.fold_in(part_splits[2], 1), 0, 1),
    }


def prototype(tap_count, chan_count):
    length = tap_count * chan_count
    position = jnp.arange(length, dtype=jnp.float32)
    centred = (position - (length - 1) / 2.0) / chan_count
    window = 0.54 - 0.46 * jnp.cos(2.0 * jnp.pi * position / (length - 1))
    shaped = jnp.sinc(centred) * window
    shaped = shaped * jnp.sqrt(chan_count / jnp.sum(shaped * shaped))
    return shaped.reshape(tap_count, chan_count)

def dedisperse(padded, delays, out_width, block_rows):
    chan_count = padded.shape[0]
    offsets = jnp.arange(out_width, dtype=jnp.int32)

    def pick_row(row_values, row_delays):
        return row_values[row_delays[:, None] + offsets[None, :]]

    def add_block(block_index, running):
        first_row = (block_index * block_rows).astype(jnp.int32)
        rows_here = lax.dynamic_slice_in_dim(padded, first_row, block_rows, 0)
        delay_here = lax.dynamic_slice_in_dim(delays, first_row, block_rows, 1)
        picked = jax.vmap(pick_row)(rows_here, delay_here.T)
        return running + lax.optimization_barrier(jnp.sum(picked.astype(jnp.float32), axis=0))
    zero_sums = jnp.zeros((delays.shape[0], out_width), jnp.float32)
    return lax.fori_loop(0, chan_count // block_rows, add_block, zero_sums)

def reference(voltage, delays, chan_mask):
    frame_count = voltage.shape[2] // NCHAN
    framed = voltage.astype(jnp.float32).reshape(2, 2, frame_count, NCHAN)
    history = jnp.zeros((2, 2, TAPS - 1, NCHAN), jnp.float32)
    extended = jnp.concatenate([history, framed], axis=2)
    coeffs = prototype(TAPS, NCHAN)
    weighted = jnp.zeros((2, 2, frame_count, NCHAN), jnp.float32)
    for tap_index in range(TAPS):
        weighted = weighted + coeffs[tap_index] * extended[:, :, tap_index:tap_index + frame_count]
    spectra = jnp.fft.fft(lax.complex(weighted[:, 0], weighted[:, 1]), axis=-1) / jnp.sqrt(jnp.float32(NCHAN))
    energy = lax.optimization_barrier(jnp.sum(jnp.real(spectra) ** 2 + jnp.imag(spectra) ** 2, axis=0))
    detected = energy.T.astype(jnp.bfloat16)
    masked = detected * chan_mask.astype(jnp.bfloat16)[:, None]
    padded = jnp.concatenate([masked, jnp.zeros((NCHAN, MAXD), jnp.bfloat16)], axis=1)
    series = dedisperse(padded, delays, frame_count, 16)
    average = lax.optimization_barrier(jnp.sum(series, axis=1)) / frame_count
    peak_value = lax.optimization_barrier(jnp.max(series, axis=1))
    centred = series - average[:, None]
    variance = lax.optimization_barrier(jnp.sum(centred * centred, axis=1)) / frame_count
    deviation = jnp.sqrt(variance + 1e-05)
    zscore = centred / deviation[:, None]
    live_count = jnp.maximum(jnp.sum(chan_mask).astype(jnp.float32), 1.0)
    trial_stats = jnp.stack([average / live_count, deviation / live_count, (peak_value - average) / deviation])
    return (zscore, trial_stats)
```

```python
import functools
import math

import jax
import jax.numpy as jnp
import numpy as np
from jax import lax
from jax.experimental import pallas as pl
from jax.experimental.pallas import tpu as pltpu
from jax.sharding import PartitionSpec as P

NCHAN = 2048
TAPS = 16
DSPAN = 3
LANES = 128
RADIX = NCHAN // LANES
BLOCK = 256
STEP = 4
MESH = pl.DeviceIdType.MESH


def prototype():
    length = TAPS * NCHAN
    position = np.arange(length, dtype=np.float64)
    window = 0.54 - 0.46 * np.cos(2.0 * np.pi * position / (length - 1))
    shaped = np.sinc((position - (length - 1) / 2.0) / NCHAN) * window
    shaped = shaped * np.sqrt(NCHAN / np.sum(shaped * shaped))
    taps = shaped.reshape(TAPS, RADIX, 1, LANES)
    taps = np.broadcast_to(taps, (TAPS, RADIX, 2, LANES))
    return taps.reshape(TAPS, 2 * RADIX, LANES).astype(np.float32)


def twiddles():
    angle = -2.0 * np.pi * np.outer(np.arange(RADIX), np.arange(LANES)) / NCHAN
    return np.stack([np.cos(angle), np.sin(angle)]).astype(np.float32)


def transform_table():
    angle = -2.0 * np.pi * (np.outer(np.arange(LANES), np.arange(LANES)) % LANES) / LANES
    scale = 1.0 / math.sqrt(NCHAN)
    cos, sin = np.cos(angle) * scale, np.sin(angle) * scale
    full = np.block([[cos, sin], [-sin, cos]]).astype(np.float32)
    high = full.astype(jnp.bfloat16)
    low = (full - high.astype(np.float32)).astype(jnp.bfloat16)
    return np.stack([high, low])


def butterflies(items):
    count = len(items)
    if count == 1:
        return items
    even = butterflies(items[0::2])
    odd = butterflies(items[1::2])
    half = count // 2
    out = [None] * count
    for k in range(half):
        re, im = odd[k]
        if k == 0:
            tr, ti = re, im
        elif 4 * k == count:
            tr, ti = im, -re
        elif 8 * k == count:
            r = math.sqrt(0.5)
            tr, ti = (re + im) * r, (im - re) * r
        elif 8 * k == 3 * count:
            r = math.sqrt(0.5)
            tr, ti = (im - re) * r, (re + im) * (-r)
        else:
            c, s = math.cos(2 * math.pi * k / count), -math.sin(2 * math.pi * k / count)
            tr, ti = re * c - im * s, re * s + im * c
        er, ei = even[k]
        out[k] = (er + tr, ei + ti)
        out[k + half] = (er - tr, ei - ti)
    return out


def channelize_kernel(frames, volt_ref, halo_ref, taps_ref, twid_ref, table_ref, mask_ref, out_ref,
                      ext, weighted, power):
    past = TAPS - 1
    lines = 2 * RADIX
    for p in range(2):
        ext[p, 0:past] = halo_ref[p].astype(jnp.float32)
        ext[p, past:past + frames] = volt_ref[p].astype(jnp.float32)
    for part in range(lines // 8):
        rows = pl.ds(8 * part, 8)
        taps = [taps_ref[j, rows, :] for j in range(TAPS)]

        def fir(f, carry):
            for p in range(2):
                terms = [taps[j] * ext[p, f + j, rows, :] for j in range(TAPS)]
                while len(terms) > 1:
                    terms = [a + b for a, b in zip(terms[0::2], terms[1::2])]
                start = pl.multiple_of((p * frames + f) * lines, 8) + 8 * part
                weighted[pl.ds(start, 8), :] = terms[0]
            return carry

        lax.fori_loop(0, frames, fir, 0, unroll=4)

    rows_all = 2 * frames
    group = 8
    high_table = table_ref[0]
    low_table = table_ref[1]
    power[...] = jnp.zeros_like(power)
    sections = [[] for _ in range(RADIX)]
    for g in range(rows_all // group):
        items = []
        for m in range(RADIX):
            pair = []
            for c in range(2):
                start = g * group * lines + 2 * m + c
                pair.append(weighted[pl.ds(start, group, stride=lines), :])
            items.append(tuple(pair))
        for k1, (re, im) in enumerate(butterflies(items)):
            if k1:
                c, s = twid_ref[0, k1:k1 + 1, :], twid_ref[1, k1:k1 + 1, :]
                re, im = re * c - im * s, re * s + im * c
            sections[k1].append(jnp.concatenate([re, im], axis=1))
    for k1 in range(RADIX):
        both = jnp.concatenate(sections[k1], axis=0)
        high = both.astype(jnp.bfloat16)
        low = (both - high.astype(jnp.float32)).astype(jnp.bfloat16)
        dot = functools.partial(jnp.dot, preferred_element_type=jnp.float32)
        spec = dot(high, high_table) + (dot(high, low_table) + dot(low, high_table))
        spec = spec * spec
        energy = spec[:, :LANES] + spec[:, LANES:]
        energy = energy[:frames] + energy[frames:]
        kept = energy.astype(jnp.bfloat16).astype(jnp.float32) * mask_ref[k1:k1 + 1, :]
        padded = jnp.concatenate([jnp.zeros((LANES - frames, LANES), jnp.float32), kept], axis=0)
        power[pl.ds(k1, LANES, stride=RADIX), :] = padded.T
    out_ref[...] = power[...].astype(jnp.bfloat16)


def dedisperse_kernel(frames, delay_ref, power_ref, out_ref, acc):
    trials = delay_ref.shape[0]
    reach = LANES - frames
    bits = max(1, reach.bit_length())
    total = jnp.zeros((trials, LANES), jnp.float32)
    for b in range(NCHAN // BLOCK):
        block = delay_ref[:, b * BLOCK:(b + 1) * BLOCK]
        base = block[:, BLOCK - 1:BLOCK]
        relative = block - base
        most = jnp.max(relative[:, 0:1])
        values = power_ref[b * BLOCK:(b + 1) * BLOCK, :]
        acc[...] = jnp.zeros_like(acc)

        def step(i, carry):
            first = i * STEP
            shifted = relative - first
            picks = [jnp.where(shifted == r, 1.0, 0.0).astype(jnp.bfloat16) for r in range(STEP)]
            sums = jnp.dot(jnp.concatenate(picks, axis=0), values, preferred_element_type=jnp.float32)
            run = sums[:trials]
            for r in range(1, STEP):
                run = run + pltpu.roll(sums[r * trials:(r + 1) * trials], LANES - r, 1)
            acc[...] += pltpu.roll(run, lax.rem(2 * LANES - first, LANES), 1)
            return carry

        lax.fori_loop(0, lax.div(most, STEP) + 1, step, 0)
        moved = acc[...]
        for bit in range(bits):
            chosen = ((base >> bit) & 1) == 1
            moved = jnp.where(chosen, pltpu.roll(moved, LANES - (1 << bit), 1), moved)
        total = total + moved
    turned = jnp.concatenate([total, jnp.zeros((LANES - trials, LANES), jnp.float32)], axis=0).T
    half = frames // 2
    for s in range(LANES // frames):
        top = turned[s * frames:s * frames + half]
        low = turned[s * frames + half:(s + 1) * frames]
        out_ref[s * half:(s + 1) * half, :] = top + pltpu.roll(low, trials, 1)


def combine_kernel(count, frames, part_ref, mask_ref, z_ref, stats_ref, landed, mine, gathered, near_send, near_recv,
                   far_send, far_recv):
    me = lax.axis_index("tm")
    half = frames // 2
    trials = LANES // 2
    barrier = pltpu.get_barrier_semaphore()
    for k in range(1, count):
        pl.semaphore_signal(barrier, inc=1, device_id={"tm": lax.rem(me + k, count)}, device_id_type=MESH)
    pl.semaphore_wait(barrier, count - 1)

    def near(k):
        return pltpu.make_async_remote_copy(
            src_ref=part_ref.at[pl.ds((DSPAN - k) * half, half)],
            dst_ref=landed.at[k - 1],
            send_sem=near_send.at[k - 1],
            recv_sem=near_recv.at[k - 1],
            device_id={"tm": me - k},
            device_id_type=MESH,
        )

    for k in range(1, DSPAN + 1):
        @pl.when(me >= k)
        def _():
            near(k).start()

        @pl.when(me < k)
        def _():
            pass

    series = part_ref[DSPAN * half:(DSPAN + 1) * half, :]
    for k in range(1, DSPAN + 1):
        @pl.when(me + k >= count)
        def _():
            landed[k - 1] = jnp.zeros((half, LANES), jnp.float32)

        @pl.when(me + k < count)
        def _():
            near(k).wait_recv()
    for k in range(1, DSPAN + 1):
        series = series + landed[k - 1]

    def fold(value, op):
        return op(value, pltpu.roll(value, trials, 1))

    mean = fold(jnp.sum(series, axis=0, keepdims=True), jnp.add) * (1.0 / frames)
    away = series - mean
    spread = fold(jnp.sum(away * away, axis=0, keepdims=True), jnp.add)
    peak = fold(jnp.max(series, axis=0, keepdims=True), jnp.maximum)
    mine[...] = jnp.concatenate([mean, spread, peak, jnp.zeros((5, LANES), jnp.float32)], axis=0)

    def far(k):
        return pltpu.make_async_remote_copy(
            src_ref=mine,
            dst_ref=gathered.at[k - 1],
            send_sem=far_send.at[k - 1],
            recv_sem=far_recv.at[k - 1],
            device_id={"tm": lax.rem(me + k, count)},
            device_id_type=MESH,
        )

    for k in range(1, count):
        far(k).start()
    live = jnp.maximum(jnp.sum(mask_ref[...].astype(jnp.float32)), 1.0)
    for k in range(1, count):
        far(k).wait_recv()
    everyone = gathered[...]
    average = (mean + jnp.sum(everyone[:, 0:1, :], axis=0)) * (1.0 / count)
    offset = everyone[:, 0:1, :] - average[None]
    squares = spread + jnp.sum(everyone[:, 1:2, :], axis=0)
    between = (mean - average) * (mean - average) + jnp.sum(offset * offset, axis=0)
    variance = (squares + frames * between) * (1.0 / (frames * count))
    top = jnp.maximum(peak, jnp.max(everyone[:, 2:3, :], axis=0))
    deviation = jnp.sqrt(variance + 1e-05)
    z = (series - average) / deviation
    z = jnp.concatenate([z, pltpu.roll(z, trials, 1), jnp.zeros((LANES - frames, LANES), jnp.float32)], axis=0).T
    z_ref[...] = z[:trials, :frames]
    stats_ref[...] = jnp.concatenate(
        [average / live, deviation / live, (top - average) / deviation], axis=0
    )[:, :trials]
    for k in range(1, DSPAN + 1):
        @pl.when(me >= k)
        def _():
            near(k).wait_send()
    for k in range(1, count):
        far(k).wait_send()


def per_device(voltage, delays, chan_mask):
    frames = voltage.shape[2] // NCHAN
    trials = delays.shape[0]
    count = lax.axis_size("tm")
    vmem = pl.BlockSpec(memory_space=pltpu.VMEM)
    lines = 2 * RADIX
    framed = voltage.reshape(2, 2, frames * RADIX, LANES).transpose(0, 2, 1, 3).reshape(2, frames, lines, LANES)
    steps = [(source, source + 1) for source in range(count - 1)]
    halo = lax.ppermute(framed[:, frames - (TAPS - 1):], "tm", steps)
    mask_table = chan_mask.astype(jnp.float32).reshape(LANES, RADIX).T
    power = pl.pallas_call(
        functools.partial(channelize_kernel, frames),
        out_shape=jax.ShapeDtypeStruct((NCHAN, LANES), jnp.bfloat16),
        in_specs=[vmem] * 6,
        out_specs=vmem,
        scratch_shapes=[
            pltpu.VMEM((2, frames + TAPS - 1, lines, LANES), jnp.float32),
            pltpu.VMEM((2 * frames * lines, LANES), jnp.float32),
            pltpu.VMEM((NCHAN, LANES), jnp.float32),
        ],
        name="channelize",
    )(framed, halo, jnp.asarray(prototype()), jnp.asarray(twiddles()), jnp.asarray(transform_table()), mask_table)
    partial = pl.pallas_call(
        functools.partial(dedisperse_kernel, frames),
        out_shape=jax.ShapeDtypeStruct((2 * trials * LANES // LANES // 2, LANES), jnp.float32),
        in_specs=[vmem] * 2,
        out_specs=vmem,
        scratch_shapes=[pltpu.VMEM((trials, LANES), jnp.float32)],
        name="dedisperse",
    )(delays, power)
    zscore, trial_stats = pl.pallas_call(
        functools.partial(combine_kernel, count, frames),
        out_shape=(
            jax.ShapeDtypeStruct((trials, frames), jnp.float32),
            jax.ShapeDtypeStruct((3, trials), jnp.float32),
        ),
        in_specs=[vmem] * 2,
        out_specs=(vmem, vmem),
        scratch_shapes=[
            pltpu.VMEM((DSPAN, frames // 2, LANES), jnp.float32),
            pltpu.VMEM((8, LANES), jnp.float32),
            pltpu.VMEM((count - 1, 8, LANES), jnp.float32),
            pltpu.SemaphoreType.DMA((DSPAN,)),
            pltpu.SemaphoreType.DMA((DSPAN,)),
            pltpu.SemaphoreType.DMA((count - 1,)),
            pltpu.SemaphoreType.DMA((count - 1,)),
        ],
        compiler_params=pltpu.CompilerParams(collective_id=0, has_side_effects=True),
        name="combine",
    )(partial, mask_table)
    return (zscore, trial_stats)


def solution(mesh):
    in_specs = (P(None, None, ("beam", "tm")), P(), P("beam"))
    out_specs = (P(None, ("beam", "tm")), P(None, "beam"))
    return jax.shard_map(
        per_device, mesh=mesh, in_specs=in_specs, out_specs=out_specs, check_vma=False
    )
```

```python
import functools
import math

import jax
import jax.numpy as jnp
import numpy as np
from jax import lax
from jax.experimental import pallas as pl
from jax.experimental.pallas import tpu as pltpu
from jax.sharding import PartitionSpec as P

NCHAN = 2048
TAPS = 16
DSPAN = 3
LANES = 128
RADIX = NCHAN // LANES
STEP = 9
MESH = pl.DeviceIdType.MESH


def prototype():
    length = TAPS * NCHAN
    position = np.arange(length, dtype=np.float64)
    window = 0.54 - 0.46 * np.cos(2.0 * np.pi * position / (length - 1))
    shaped = np.sinc((position - (length - 1) / 2.0) / NCHAN) * window
    shaped = shaped * np.sqrt(NCHAN / np.sum(shaped * shaped))
    taps = shaped.reshape(TAPS, RADIX, 1, LANES)
    taps = np.broadcast_to(taps, (TAPS, RADIX, 2, LANES))
    return taps.reshape(TAPS, 2 * RADIX, LANES).astype(np.float32)


def twiddles():
    angle = -2.0 * np.pi * np.outer(np.arange(RADIX), np.arange(LANES)) / NCHAN
    return np.stack([np.cos(angle), np.sin(angle)]).astype(np.float32)


def transform_table():
    angle = -2.0 * np.pi * (np.outer(np.arange(LANES), np.arange(LANES)) % LANES) / LANES
    scale = 1.0 / math.sqrt(NCHAN)
    cos, sin = np.cos(angle) * scale, np.sin(angle) * scale
    full = np.block([[cos, sin], [-sin, cos]]).astype(np.float32)
    high = full.astype(jnp.bfloat16)
    low = (full - high.astype(np.float32)).astype(jnp.bfloat16)
    return np.stack([high, low])


def butterflies(items):
    count = len(items)
    if count == 1:
        return items
    even = butterflies(items[0::2])
    odd = butterflies(items[1::2])
    half = count // 2
    out = [None] * count
    for k in range(half):
        re, im = odd[k]
        if k == 0:
            tr, ti = re, im
        elif 4 * k == count:
            tr, ti = im, -re
        elif 8 * k == count:
            r = math.sqrt(0.5)
            tr, ti = (re + im) * r, (im - re) * r
        elif 8 * k == 3 * count:
            r = math.sqrt(0.5)
            tr, ti = (im - re) * r, (re + im) * (-r)
        else:
            c, s = math.cos(2 * math.pi * k / count), -math.sin(2 * math.pi * k / count)
            tr, ti = re * c - im * s, re * s + im * c
        er, ei = even[k]
        out[k] = (er + tr, ei + ti)
        out[k + half] = (er - tr, ei - ti)
    return out


def channelize_kernel(count, frames, volt_ref, taps_ref, twid_ref, table_ref, out_ref,
                      halo, ext, weighted, sections, energy, power, send_sem, recv_sem):
    me = lax.axis_index("tm")
    past = TAPS - 1
    lines = 2 * RADIX
    half = frames // 2
    barrier = pltpu.get_barrier_semaphore()

    def pass_on():
        return pltpu.make_async_remote_copy(
            src_ref=volt_ref.at[:, pl.ds(frames - past, past)],
            dst_ref=halo,
            send_sem=send_sem,
            recv_sem=recv_sem,
            device_id={"tm": me + 1},
            device_id_type=MESH,
        )

    @pl.when(me > 0)
    def _():
        pl.semaphore_signal(barrier, inc=1, device_id={"tm": me - 1}, device_id_type=MESH)

    @pl.when(me < count - 1)
    def _():
        pl.semaphore_wait(barrier, 1)
        pass_on().start()

    for p in range(2):
        ext[p, past:past + frames] = volt_ref[p].astype(jnp.float32)

    def fir(begin, end):
        for part in range(lines // 8):
            rows = pl.ds(8 * part, 8)
            taps = [taps_ref[j, rows, :] for j in range(TAPS)]

            def one(f, carry):
                for p in range(2):
                    terms = [taps[j] * ext[p, f + j, rows, :] for j in range(TAPS)]
                    while len(terms) > 1:
                        terms = [a + b for a, b in zip(terms[0::2], terms[1::2])]
                    start = pl.multiple_of((p * frames + f) * lines, 8) + 8 * part
                    weighted[pl.ds(start, 8), :] = terms[0]
                return carry

            lax.fori_loop(begin, end, one, 0, unroll=4)

    def transform(begin):
        group = 8
        rows_half = 2 * half
        for g in range(rows_half // group):
            p, f = divmod(g * group, half)
            first = (p * frames + begin + f) * lines
            items = []
            for m in range(RADIX):
                re = weighted[pl.ds(first + 2 * m, group, stride=lines), :]
                im = weighted[pl.ds(first + 2 * m + 1, group, stride=lines), :]
                items.append((re, im))
            for k1, (re, im) in enumerate(butterflies(items)):
                if k1:
                    c, s = twid_ref[0, k1:k1 + 1, :], twid_ref[1, k1:k1 + 1, :]
                    re, im = re * c - im * s, re * s + im * c
                place = k1 * rows_half + g * group
                sections[place:place + group, :LANES] = re
                sections[place:place + group, LANES:] = im
        both = sections[...]
        high = both.astype(jnp.bfloat16)
        low = (both - high.astype(jnp.float32)).astype(jnp.bfloat16)
        dot = functools.partial(jnp.dot, preferred_element_type=jnp.float32)
        spec = dot(high, table_ref[0]) + (dot(high, table_ref[1]) + dot(low, table_ref[0]))
        spec = spec * spec
        both_pols = (spec[:, :LANES] + spec[:, LANES:]).reshape(RADIX, 2, half, LANES)
        energy[:, begin:begin + half, :] = both_pols[:, 0] + both_pols[:, 1]

    fir(half, frames)
    transform(half)

    @pl.when(me > 0)
    def _():
        pass_on().wait_recv()
        for p in range(2):
            ext[p, 0:past] = halo[p].astype(jnp.float32)

    @pl.when(me == 0)
    def _():
        for p in range(2):
            ext[p, 0:past] = jnp.zeros((past, lines, LANES), jnp.float32)

    fir(0, half)
    transform(0)
    for k1 in range(RADIX):
        padded = jnp.concatenate([jnp.zeros((LANES - frames, LANES), jnp.float32), energy[k1]], axis=0)
        power[pl.ds(k1, LANES, stride=RADIX), :] = padded.T
    out_ref[...] = power[...].astype(jnp.bfloat16)

    @pl.when(me < count - 1)
    def _():
        pass_on().wait_send()


def dedisperse_kernel(frames, delay_ref, mask_ref, power_ref, out_ref, relative, acc):
    trials = delay_ref.shape[0]
    reach = LANES - frames
    bits = max(1, reach.bit_length())
    blocks = NCHAN // LANES
    bases = []
    most = jnp.zeros((trials, 1), jnp.int32)
    for b in range(blocks):
        block = delay_ref[:, b * LANES:(b + 1) * LANES]
        base = block[:, LANES - 1:LANES]
        bases.append(base)
        away = block - base
        most = jnp.maximum(most, away[:, 0:1])
        away = jnp.where(mask_ref[b:b + 1, :] > 0, away, -1)
        relative[:, b * LANES:(b + 1) * LANES] = away.astype(jnp.float32).astype(jnp.bfloat16)
    zeros = jnp.zeros((LANES, LANES), jnp.bfloat16)

    def sweep(first, pair):
        upper = power_ref[2 * pair * LANES:(2 * pair + 1) * LANES, :]
        lower = power_ref[(2 * pair + 1) * LANES:(2 * pair + 2) * LANES, :]
        values = jnp.concatenate(
            [jnp.concatenate([upper, zeros], axis=1), jnp.concatenate([zeros, lower], axis=1)], axis=0
        )
        away = relative[:, 2 * pair * LANES:(2 * pair + 2) * LANES]
        picks = []
        for r in range(STEP):
            target = jnp.asarray(first + r, jnp.float32).astype(jnp.bfloat16)
            picks.append(jnp.where(away == target, jnp.ones_like(away), jnp.zeros_like(away)))
        sums = jnp.dot(jnp.concatenate(picks, axis=0), values, preferred_element_type=jnp.float32)
        out = []
        for side in range(2):
            part = sums[:, side * LANES:(side + 1) * LANES]
            run = part[:trials]
            for r in range(1, STEP):
                run = run + pltpu.roll(part[r * trials:(r + 1) * trials], LANES - r, 1)
            out.append(run)
        return out

    for pair in range(blocks // 2):
        for side, run in enumerate(sweep(0, pair)):
            acc[2 * pair + side] = run

    def more(i, carry):
        first = i * STEP
        turn = lax.rem(2 * LANES - first, LANES)
        for pair in range(blocks // 2):
            for side, run in enumerate(sweep(first, pair)):
                acc[2 * pair + side] += pltpu.roll(run, turn, 1)
        return carry

    lax.fori_loop(1, lax.div(jnp.max(most), STEP) + 1, more, 0)
    total = jnp.zeros((trials, LANES), jnp.float32)
    for b in range(blocks):
        moved = acc[b]
        for bit in range(bits):
            chosen = ((bases[b] >> bit) & 1) == 1
            moved = jnp.where(chosen, pltpu.roll(moved, LANES - (1 << bit), 1), moved)
        total = total + moved
    turned = jnp.concatenate([total, jnp.zeros((LANES - trials, LANES), jnp.float32)], axis=0).T
    half = frames // 2
    for s in range(LANES // frames):
        top = turned[s * frames:s * frames + half]
        low = turned[s * frames + half:(s + 1) * frames]
        out_ref[s * half:(s + 1) * half, :] = top + pltpu.roll(low, trials, 1)


def combine_kernel(count, frames, part_ref, mask_ref, z_ref, stats_ref, landed, mine, gathered, near_send, near_recv,
                   far_send, far_recv):
    me = lax.axis_index("tm")
    half = frames // 2
    trials = LANES // 2
    barrier = pltpu.get_barrier_semaphore()
    for k in range(1, count):
        pl.semaphore_signal(barrier, inc=1, device_id={"tm": lax.rem(me + k, count)}, device_id_type=MESH)
    pl.semaphore_wait(barrier, count - 1)

    def near(k):
        return pltpu.make_async_remote_copy(
            src_ref=part_ref.at[pl.ds((DSPAN - k) * half, half)],
            dst_ref=landed.at[k - 1],
            send_sem=near_send.at[k - 1],
            recv_sem=near_recv.at[k - 1],
            device_id={"tm": me - k},
            device_id_type=MESH,
        )

    for k in range(1, DSPAN + 1):
        @pl.when(me >= k)
        def _():
            near(k).start()

    series = part_ref[DSPAN * half:(DSPAN + 1) * half, :]
    for k in range(1, DSPAN + 1):
        @pl.when(me + k >= count)
        def _():
            landed[k - 1] = jnp.zeros((half, LANES), jnp.float32)

        @pl.when(me + k < count)
        def _():
            near(k).wait_recv()
    for k in range(1, DSPAN + 1):
        series = series + landed[k - 1]

    def fold(value, op):
        return op(value, pltpu.roll(value, trials, 1))

    mean = fold(jnp.sum(series, axis=0, keepdims=True), jnp.add) * (1.0 / frames)
    away = series - mean
    spread = fold(jnp.sum(away * away, axis=0, keepdims=True), jnp.add)
    peak = fold(jnp.max(series, axis=0, keepdims=True), jnp.maximum)
    mine[...] = jnp.concatenate([mean, spread, peak, jnp.zeros((5, LANES), jnp.float32)], axis=0)

    def far(k):
        return pltpu.make_async_remote_copy(
            src_ref=mine,
            dst_ref=gathered.at[k - 1],
            send_sem=far_send.at[k - 1],
            recv_sem=far_recv.at[k - 1],
            device_id={"tm": lax.rem(me + k, count)},
            device_id_type=MESH,
        )

    for k in range(1, count):
        far(k).start()
    live = jnp.maximum(jnp.sum(mask_ref[...].astype(jnp.float32)), 1.0)
    for k in range(1, count):
        far(k).wait_recv()
    everyone = gathered[...]
    average = (mean + jnp.sum(everyone[:, 0:1, :], axis=0)) * (1.0 / count)
    offset = everyone[:, 0:1, :] - average[None]
    squares = spread + jnp.sum(everyone[:, 1:2, :], axis=0)
    between = (mean - average) * (mean - average) + jnp.sum(offset * offset, axis=0)
    variance = (squares + frames * between) * (1.0 / (frames * count))
    top = jnp.maximum(peak, jnp.max(everyone[:, 2:3, :], axis=0))
    deviation = jnp.sqrt(variance + 1e-05)
    z = (series - average) / deviation
    z_ref[0:half, :] = z[:, :trials]
    z_ref[half:frames, :] = pltpu.roll(z, trials, 1)[:, :trials]
    stats_ref[...] = jnp.concatenate(
        [average / live, deviation / live, (top - average) / deviation], axis=0
    )[:, :trials]
    for k in range(1, DSPAN + 1):
        @pl.when(me >= k)
        def _():
            near(k).wait_send()
    for k in range(1, count):
        far(k).wait_send()


def per_device(voltage, delays, chan_mask):
    frames = voltage.shape[2] // NCHAN
    trials = delays.shape[0]
    count = lax.axis_size("tm")
    vmem = pl.BlockSpec(memory_space=pltpu.VMEM)
    lines = 2 * RADIX
    framed = voltage.reshape(2, 2, frames * RADIX, LANES).transpose(0, 2, 1, 3).reshape(2, frames, lines, LANES)
    mask_table = chan_mask.reshape(RADIX, LANES)
    power = pl.pallas_call(
        functools.partial(channelize_kernel, count, frames),
        out_shape=jax.ShapeDtypeStruct((NCHAN, LANES), jnp.bfloat16),
        in_specs=[vmem] * 4,
        out_specs=vmem,
        scratch_shapes=[
            pltpu.VMEM((2, TAPS - 1, lines, LANES), jnp.bfloat16),
            pltpu.VMEM((2, frames + TAPS - 1, lines, LANES), jnp.float32),
            pltpu.VMEM((2 * frames * lines, LANES), jnp.float32),
            pltpu.VMEM((RADIX * frames, 2 * LANES), jnp.float32),
            pltpu.VMEM((RADIX, frames, LANES), jnp.float32),
            pltpu.VMEM((NCHAN, LANES), jnp.float32),
            pltpu.SemaphoreType.DMA,
            pltpu.SemaphoreType.DMA,
        ],
        compiler_params=pltpu.CompilerParams(collective_id=1, has_side_effects=True),
        name="channelize",
    )(framed, jnp.asarray(prototype()), jnp.asarray(twiddles()), jnp.asarray(transform_table()))
    partial = pl.pallas_call(
        functools.partial(dedisperse_kernel, frames),
        out_shape=jax.ShapeDtypeStruct((2 * frames, LANES), jnp.float32),
        in_specs=[vmem] * 3,
        out_specs=vmem,
        scratch_shapes=[
            pltpu.VMEM((trials, NCHAN), jnp.bfloat16),
            pltpu.VMEM((NCHAN // LANES, trials, LANES), jnp.float32),
        ],
        name="dedisperse",
    )(delays, mask_table, power)
    zscore, trial_stats = pl.pallas_call(
        functools.partial(combine_kernel, count, frames),
        out_shape=(
            jax.ShapeDtypeStruct((frames, trials), jnp.float32),
            jax.ShapeDtypeStruct((3, trials), jnp.float32),
        ),
        in_specs=[vmem] * 2,
        out_specs=(vmem, vmem),
        scratch_shapes=[
            pltpu.VMEM((DSPAN, frames // 2, LANES), jnp.float32),
            pltpu.VMEM((8, LANES), jnp.float32),
            pltpu.VMEM((count - 1, 8, LANES), jnp.float32),
            pltpu.SemaphoreType.DMA((DSPAN,)),
            pltpu.SemaphoreType.DMA((DSPAN,)),
            pltpu.SemaphoreType.DMA((count - 1,)),
            pltpu.SemaphoreType.DMA((count - 1,)),
        ],
        compiler_params=pltpu.CompilerParams(collective_id=0, has_side_effects=True),
        name="combine",
    )(partial, mask_table)
    return (zscore.T, trial_stats)


def solution(mesh):
    in_specs = (P(None, None, ("beam", "tm")), P(), P("beam"))
    out_specs = (P(None, ("beam", "tm")), P(None, "beam"))
    return jax.shard_map(
        per_device, mesh=mesh, in_specs=in_specs, out_specs=out_specs, check_vma=False
    )
```

```python
import functools
import math

import jax
import jax.numpy as jnp
import numpy as np
from jax import lax
from jax.experimental import pallas as pl
from jax.experimental.pallas import tpu as pltpu
from jax.sharding import PartitionSpec as P

NCHAN = 2048
TAPS = 16
DSPAN = 3
LANES = 128
RADIX = NCHAN // LANES
STEP = 9
GRANT = 16 * 1024 * 1024
MESH = pl.DeviceIdType.MESH


def prototype():
    length = TAPS * NCHAN
    position = np.arange(length, dtype=np.float64)
    window = 0.54 - 0.46 * np.cos(2.0 * np.pi * position / (length - 1))
    shaped = np.sinc((position - (length - 1) / 2.0) / NCHAN) * window
    shaped = shaped * np.sqrt(NCHAN / np.sum(shaped * shaped))
    taps = shaped.reshape(TAPS, RADIX, 1, LANES)
    taps = np.broadcast_to(taps, (TAPS, RADIX, 2, LANES))
    return taps.reshape(TAPS, 2 * RADIX, LANES).astype(np.float32)


def twiddles():
    angle = -2.0 * np.pi * np.outer(np.arange(RADIX), np.arange(LANES)) / NCHAN
    return np.stack([np.cos(angle), np.sin(angle)]).astype(np.float32)


def transform_table():
    angle = -2.0 * np.pi * (np.outer(np.arange(LANES), np.arange(LANES)) % LANES) / LANES
    scale = 1.0 / math.sqrt(NCHAN)
    cos, sin = np.cos(angle) * scale, np.sin(angle) * scale
    full = np.block([[cos, sin], [-sin, cos]]).astype(np.float32)
    high = full.astype(jnp.bfloat16)
    low = (full - high.astype(np.float32)).astype(jnp.bfloat16)
    return np.stack([high, low])


def butterflies(items):
    count = len(items)
    if count == 1:
        return items
    even = butterflies(items[0::2])
    odd = butterflies(items[1::2])
    half = count // 2
    out = [None] * count
    for k in range(half):
        re, im = odd[k]
        if k == 0:
            tr, ti = re, im
        elif 4 * k == count:
            tr, ti = im, -re
        elif 8 * k == count:
            r = math.sqrt(0.5)
            tr, ti = (re + im) * r, (im - re) * r
        elif 8 * k == 3 * count:
            r = math.sqrt(0.5)
            tr, ti = (im - re) * r, (re + im) * (-r)
        else:
            c, s = math.cos(2 * math.pi * k / count), -math.sin(2 * math.pi * k / count)
            tr, ti = re * c - im * s, re * s + im * c
        er, ei = even[k]
        out[k] = (er + tr, ei + ti)
        out[k + half] = (er - tr, ei - ti)
    return out


def channelize_kernel(count, frames, volt_ref, taps_ref, twid_ref, table_ref, delay_ref, mask_ref, out_ref,
                      relative_ref, meta_ref, halo, ext, weighted, sections, energy, power, send_sem, recv_sem):
    me = lax.axis_index("tm")
    past = TAPS - 1
    lines = 2 * RADIX
    half = frames // 2
    quarter = frames // 4
    cut = min(quarter, past - 1)
    spans = ((cut, past - cut), (0, cut))
    barrier = pltpu.get_barrier_semaphore()

    def pass_on(i):
        begin, size = spans[i]
        return pltpu.make_async_remote_copy(
            src_ref=volt_ref.at[:, pl.ds(frames - past + begin, size)],
            dst_ref=halo.at[:, pl.ds(begin, size)],
            send_sem=send_sem.at[i],
            recv_sem=recv_sem.at[i],
            device_id={"tm": me + 1},
            device_id_type=MESH,
        )

    @pl.when(me > 0)
    def _():
        pl.semaphore_signal(barrier, inc=1, device_id={"tm": me - 1}, device_id_type=MESH)

    @pl.when(me < count - 1)
    def _():
        pl.semaphore_wait(barrier, 1)
        pass_on(0).start()
        pass_on(1).start()

    for p in range(2):
        ext[p, past:past + frames] = volt_ref[p].astype(jnp.float32)

    def fir(begin, end):
        for part in range(lines // 8):
            rows = pl.ds(8 * part, 8)
            taps = [taps_ref[j, rows, :] for j in range(TAPS)]

            def one(f, carry):
                for p in range(2):
                    terms = [taps[j] * ext[p, f + j, rows, :] for j in range(TAPS)]
                    while len(terms) > 1:
                        terms = [a + b for a, b in zip(terms[0::2], terms[1::2])]
                    start = pl.multiple_of((p * frames + f) * lines, 8) + 8 * part
                    weighted[pl.ds(start, 8), :] = terms[0]
                return carry

            lax.fori_loop(begin, end, one, 0, unroll=4)

    def transform(begin, size):
        group = 8
        rows_half = 2 * size
        for g in range(rows_half // group):
            p, f = divmod(g * group, size)
            first = (p * frames + begin + f) * lines
            items = []
            for m in range(RADIX):
                re = weighted[pl.ds(first + 2 * m, group, stride=lines), :]
                im = weighted[pl.ds(first + 2 * m + 1, group, stride=lines), :]
                items.append((re, im))
            for k1, (re, im) in enumerate(butterflies(items)):
                if k1:
                    c, s = twid_ref[0, k1:k1 + 1, :], twid_ref[1, k1:k1 + 1, :]
                    re, im = re * c - im * s, re * s + im * c
                place = k1 * rows_half + g * group
                sections[place:place + group, :LANES] = re
                sections[place:place + group, LANES:] = im
        both = sections[0:RADIX * rows_half, :]
        high = both.astype(jnp.bfloat16)
        low = (both - high.astype(jnp.float32)).astype(jnp.bfloat16)
        dot = functools.partial(jnp.dot, preferred_element_type=jnp.float32)
        spec = dot(high, table_ref[0]) + (dot(high, table_ref[1]) + dot(low, table_ref[0]))
        spec = spec * spec
        both_pols = (spec[:, :LANES] + spec[:, LANES:]).reshape(RADIX, 2, size, LANES)
        energy[:, begin:begin + size, :] = both_pols[:, 0] + both_pols[:, 1]

    fir(half, frames)
    transform(half, frames - half)
    trials = delay_ref.shape[0]
    blocks = NCHAN // LANES
    lane = lax.broadcasted_iota(jnp.int32, (trials, LANES), 1)
    meta = jnp.zeros((trials, LANES), jnp.int32)
    most = jnp.zeros((trials, 1), jnp.int32)
    for b in range(blocks):
        block = delay_ref[:, b * LANES:(b + 1) * LANES]
        base = block[:, LANES - 1:LANES]
        away = block - base
        most = jnp.maximum(most, away[:, 0:1])
        meta = jnp.where(lane == b, base, meta)
        away = jnp.where(mask_ref[b:b + 1, :] > 0, away, -1)
        relative_ref[:, b * LANES:(b + 1) * LANES] = away.astype(jnp.float32).astype(jnp.bfloat16)
    meta_ref[...] = jnp.where(lane == blocks, most, meta)

    for i, (begin, end) in enumerate(((quarter, half), (0, quarter))):
        first, size = spans[i]

        @pl.when(me > 0)
        def _():
            pass_on(i).wait_recv()
            for p in range(2):
                ext[p, first:first + size] = halo[p, first:first + size].astype(jnp.float32)

        @pl.when(me == 0)
        def _():
            for p in range(2):
                ext[p, first:first + size] = jnp.zeros((size, lines, LANES), jnp.float32)

        fir(begin, end)
        transform(begin, end - begin)

    for k1 in range(RADIX):
        padded = jnp.concatenate([jnp.zeros((LANES - frames, LANES), jnp.float32), energy[k1]], axis=0)
        power[pl.ds(k1, LANES, stride=RADIX), :] = padded.T
    out_ref[...] = power[...].astype(jnp.bfloat16)

    @pl.when(me < count - 1)
    def _():
        pass_on(0).wait_send()
        pass_on(1).wait_send()


def dedisperse_kernel(frames, relative, meta_ref, power_ref, out_ref, acc):
    trials = relative.shape[0]
    blocks = NCHAN // LANES
    most = meta_ref[:, blocks:blocks + 1]
    zeros = jnp.zeros((LANES, LANES), jnp.bfloat16)

    def sweep(first, pair):
        upper = power_ref[2 * pair * LANES:(2 * pair + 1) * LANES, :]
        lower = power_ref[(2 * pair + 1) * LANES:(2 * pair + 2) * LANES, :]
        values = jnp.concatenate(
            [jnp.concatenate([upper, zeros], axis=1), jnp.concatenate([zeros, lower], axis=1)], axis=0
        )
        away = relative[:, 2 * pair * LANES:(2 * pair + 2) * LANES]
        picks = []
        for r in range(STEP):
            target = jnp.asarray(first + r, jnp.float32).astype(jnp.bfloat16)
            picks.append(jnp.where(away == target, jnp.ones_like(away), jnp.zeros_like(away)))
        sums = jnp.dot(jnp.concatenate(picks, axis=0), values, preferred_element_type=jnp.float32)
        out = []
        for side in range(2):
            part = sums[:, side * LANES:(side + 1) * LANES]
            run = part[:trials]
            for r in range(1, STEP):
                run = run + pltpu.roll(part[r * trials:(r + 1) * trials], LANES - r, 1)
            out.append(run)
        return out

    for pair in range(blocks // 2):
        for side, run in enumerate(sweep(0, pair)):
            acc[2 * pair + side] = run

    def more(i, carry):
        first = i * STEP
        turn = lax.rem(2 * LANES - first, LANES)
        for pair in range(blocks // 2):
            for side, run in enumerate(sweep(first, pair)):
                acc[2 * pair + side] += pltpu.roll(run, turn, 1)
        return carry

    lax.fori_loop(1, lax.div(jnp.max(most), STEP) + 1, more, 0)
    lane = lax.broadcasted_iota(jnp.int32, (trials, LANES), 1)
    total = jnp.zeros((trials, LANES), jnp.float32)
    for b in range(blocks):
        place = (lane + meta_ref[:, b:b + 1]) & (LANES - 1)
        total = total + jnp.take_along_axis(acc[b], place, axis=1, mode="promise_in_bounds")
    turned = jnp.concatenate([total, jnp.zeros((LANES - trials, LANES), jnp.float32)], axis=0).T
    half = frames // 2
    for s in range(LANES // frames):
        top = turned[s * frames:s * frames + half]
        low = turned[s * frames + half:(s + 1) * frames]
        out_ref[s * half:(s + 1) * half, :] = top + pltpu.roll(low, trials, 1)


def combine_kernel(count, frames, part_ref, mask_ref, z_ref, stats_ref, landed, mine, gathered, near_send, near_recv,
                   far_send, far_recv):
    me = lax.axis_index("tm")
    half = frames // 2
    trials = LANES // 2
    barrier = pltpu.get_barrier_semaphore()
    for k in range(1, count):
        pl.semaphore_signal(barrier, inc=1, device_id={"tm": lax.rem(me + k, count)}, device_id_type=MESH)
    pl.semaphore_wait(barrier, count - 1)

    def near(k):
        return pltpu.make_async_remote_copy(
            src_ref=part_ref.at[pl.ds((DSPAN - k) * half, half)],
            dst_ref=landed.at[k - 1],
            send_sem=near_send.at[k - 1],
            recv_sem=near_recv.at[k - 1],
            device_id={"tm": me - k},
            device_id_type=MESH,
        )

    for k in range(1, DSPAN + 1):
        @pl.when(me >= k)
        def _():
            near(k).start()

    series = part_ref[DSPAN * half:(DSPAN + 1) * half, :]
    for k in range(1, DSPAN + 1):
        @pl.when(me + k >= count)
        def _():
            landed[k - 1] = jnp.zeros((half, LANES), jnp.float32)

        @pl.when(me + k < count)
        def _():
            near(k).wait_recv()
    for k in range(1, DSPAN + 1):
        series = series + landed[k - 1]

    def fold(value, op):
        return op(value, pltpu.roll(value, trials, 1))

    mean = fold(jnp.sum(series, axis=0, keepdims=True), jnp.add) * (1.0 / frames)
    away = series - mean
    spread = fold(jnp.sum(away * away, axis=0, keepdims=True), jnp.add)
    peak = fold(jnp.max(series, axis=0, keepdims=True), jnp.maximum)
    mine[...] = jnp.concatenate([mean, spread, peak, jnp.zeros((5, LANES), jnp.float32)], axis=0)

    def far(k):
        return pltpu.make_async_remote_copy(
            src_ref=mine,
            dst_ref=gathered.at[k - 1],
            send_sem=far_send.at[k - 1],
            recv_sem=far_recv.at[k - 1],
            device_id={"tm": lax.rem(me + k, count)},
            device_id_type=MESH,
        )

    for k in range(1, count):
        far(k).start()
    live = jnp.maximum(jnp.sum(mask_ref[...].astype(jnp.float32)), 1.0)
    for k in range(1, count):
        far(k).wait_recv()
    everyone = gathered[...]
    average = (mean + jnp.sum(everyone[:, 0:1, :], axis=0)) * (1.0 / count)
    offset = everyone[:, 0:1, :] - average[None]
    squares = spread + jnp.sum(everyone[:, 1:2, :], axis=0)
    between = (mean - average) * (mean - average) + jnp.sum(offset * offset, axis=0)
    variance = (squares + frames * between) * (1.0 / (frames * count))
    top = jnp.maximum(peak, jnp.max(everyone[:, 2:3, :], axis=0))
    deviation = jnp.sqrt(variance + 1e-05)
    z = (series - average) / deviation
    z_ref[0:half, :] = z[:, :trials]
    z_ref[half:frames, :] = pltpu.roll(z, trials, 1)[:, :trials]
    stats_ref[...] = jnp.concatenate(
        [average / live, deviation / live, (top - average) / deviation], axis=0
    )[:, :trials]
    for k in range(1, DSPAN + 1):
        @pl.when(me >= k)
        def _():
            near(k).wait_send()
    for k in range(1, count):
        far(k).wait_send()


def per_device(voltage, delays, chan_mask):
    frames = voltage.shape[2] // NCHAN
    trials = delays.shape[0]
    count = lax.axis_size("tm")
    vmem = pl.BlockSpec(memory_space=pltpu.VMEM)
    lines = 2 * RADIX
    framed = voltage.reshape(2, 2, frames * RADIX, LANES).transpose(0, 2, 1, 3).reshape(2, frames, lines, LANES)
    mask_table = chan_mask.reshape(RADIX, LANES)
    power, relative, meta = pl.pallas_call(
        functools.partial(channelize_kernel, count, frames),
        out_shape=(
            jax.ShapeDtypeStruct((NCHAN, LANES), jnp.bfloat16),
            jax.ShapeDtypeStruct((trials, NCHAN), jnp.bfloat16),
            jax.ShapeDtypeStruct((trials, LANES), jnp.int32),
        ),
        in_specs=[vmem] * 6,
        out_specs=(vmem,) * 3,
        scratch_shapes=[
            pltpu.VMEM((2, TAPS - 1, lines, LANES), jnp.bfloat16),
            pltpu.VMEM((2, frames + TAPS - 1, lines, LANES), jnp.float32),
            pltpu.VMEM((2 * frames * lines, LANES), jnp.float32),
            pltpu.VMEM((RADIX * frames, 2 * LANES), jnp.float32),
            pltpu.VMEM((RADIX, frames, LANES), jnp.float32),
            pltpu.VMEM((NCHAN, LANES), jnp.float32),
            pltpu.SemaphoreType.DMA((2,)),
            pltpu.SemaphoreType.DMA((2,)),
        ],
        compiler_params=pltpu.CompilerParams(collective_id=1, vmem_limit_bytes=GRANT, has_side_effects=True),
        name="channelize",
    )(framed, jnp.asarray(prototype()), jnp.asarray(twiddles()), jnp.asarray(transform_table()), delays, mask_table)
    partial = pl.pallas_call(
        functools.partial(dedisperse_kernel, frames),
        out_shape=jax.ShapeDtypeStruct((2 * frames, LANES), jnp.float32),
        in_specs=[vmem] * 3,
        out_specs=vmem,
        scratch_shapes=[
            pltpu.VMEM((NCHAN // LANES, trials, LANES), jnp.float32),
        ],
        compiler_params=pltpu.CompilerParams(vmem_limit_bytes=GRANT),
        name="dedisperse",
    )(relative, meta, power)
    zscore, trial_stats = pl.pallas_call(
        functools.partial(combine_kernel, count, frames),
        out_shape=(
            jax.ShapeDtypeStruct((frames, trials), jnp.float32),
            jax.ShapeDtypeStruct((3, trials), jnp.float32),
        ),
        in_specs=[vmem] * 2,
        out_specs=(vmem, vmem),
        scratch_shapes=[
            pltpu.VMEM((DSPAN, frames // 2, LANES), jnp.float32),
            pltpu.VMEM((8, LANES), jnp.float32),
            pltpu.VMEM((count - 1, 8, LANES), jnp.float32),
            pltpu.SemaphoreType.DMA((DSPAN,)),
            pltpu.SemaphoreType.DMA((DSPAN,)),
            pltpu.SemaphoreType.DMA((count - 1,)),
            pltpu.SemaphoreType.DMA((count - 1,)),
        ],
        compiler_params=pltpu.CompilerParams(collective_id=0, vmem_limit_bytes=GRANT, has_side_effects=True),
        name="combine",
    )(partial, mask_table)
    return (zscore.T, trial_stats)


def solution(mesh):
    in_specs = (P(None, None, ("beam", "tm")), P(), P("beam"))
    out_specs = (P(None, ("beam", "tm")), P(None, "beam"))
    return jax.shard_map(
        per_device, mesh=mesh, in_specs=in_specs, out_specs=out_specs, check_vma=False
    )
```
